256 devices in a mesh: wide: 64 (over y, z_hi, x), narrow: 4 (over z_lo, core).
Axes of the slice: x: 4, y: 4, z: 8 (z_hi: 4, z_lo: 2; z = z_hi * 2 + z_lo), core: 2. Of those that a mesh axis runs over, the one named last changes fastest.
Arguments:
- value_in: float32 [128, 16, 16, 512], P('wide', None, None, 'narrow'), may hold values from -6 to 6
- payoff: float32 [128, 16, 16, 512], P('wide', None, None, 'narrow'), may hold values from -6 to 6
- diffusion: float32 [4, 128, 16, 16, 512], P(None, 'wide', None, None, 'narrow'), may hold values from 0.25 to 2
- cross_terms: float32 [6, 128, 16, 16, 512], P(None, 'wide', None, None, 'narrow'), may hold values from -0.3 to 0.3
- flags: int32 [1, 128, 16, 16, 512], P(None, 'wide', None, None, 'narrow'), may hold values 0 or 1
- cotangent: float32 [128, 16, 16, 512], P('wide', None, None, 'narrow'), may hold values from -6 to 6
Outputs:
- grad_value: float32 [128, 16, 16, 512], P('wide', None, None, 'narrow')
- grad_payoff: float32 [128, 16, 16, 512], P('wide', None, None, 'narrow')
- grad_diffusion: float32 [4, 128, 16, 16, 512], P(None, 'wide', None, None, 'narrow')
- grad_cross: float32 [6, 128, 16, 16, 512], P(None, 'wide', None, None, 'narrow')
The draws below stay inside these ranges and needn't reach their ends.
All inputs are finite; a program needn't handle non-finite values. No bound on the sum of `flags` on one device may be relied on, other than what follows from the above.
Results may differ from the reference program's by a relative error of at most 0.00002.
Values sent between devices are 32-bit elements; how exact they have to be, the bound alone decides.
No kernel may reach another device: no remote copies, remote signals or barrier semaphores. Data moves between devices by JAX's collectives and lax.ppermute only.
A program may use at most 192 MiB of HBM per device.

```python
import math
import jax
import jax.numpy as jnp
from jax import lax

N1 = 16
N2 = 16
STEPS = 1
SWEEPS = 2
N0 = 128
N3 = 512


def touch_ends(array, own_key, smallest, top_value):
    longest = array.shape.index(max(array.shape))
    spots = []
    for shift in (0, 1):
        where = [jax.random.randint(jax.random.fold_in(own_key, axis), (), 0, length) for axis, length in enumerate(array.shape)]
        where[longest] = (where[longest] + shift) % array.shape[longest]
        spots.append(tuple(where))
    return array.at[spots[0]].set(smallest).at[spots[1]].set(top_value)


def levels(rng, dims, pieces, least, largest):
    gain, own = 1.0, jax.random.fold_in(rng, 6)
    for axis_at, parts in pieces:
        steps = jnp.exp(jax.random.uniform(jax.random.fold_in(own, axis_at), (parts,), jnp.float32, least / len(pieces), largest / len(pieces)))
        gain = gain * jnp.repeat(steps, dims[axis_at] // parts).reshape([-1 if axis == axis_at else 1 for axis in range(len(dims))])
    return gain


def centred(own_key, extent, deviation, most, split=(), dtype=jnp.bfloat16):
    drawn = jax.random.normal(own_key, extent, jnp.float32) * deviation
    if len(split) > 0:
        drawn = levels(own_key, extent, split, -0.22, 0.18) * drawn
    return jnp.clip(drawn, min=-most, max=most).astype(dtype)


def setup_inputs(seed: int = 0) -> dict:
    keys = jax.random.split(jax.random.key(seed), 7)
    return {
        "value_in": centred(keys[0], (N0, N1, N2, N3), 1.0, 6.0, ((0, 64), (3, 4)), jnp.float32),
        "payoff": centred(keys[1], (N0, N1, N2, N3), 1.0, 6.0, ((0, 64), (3, 4)), jnp.float32),
        "diffusion": jnp.clip(jnp.exp(math.log(2.0) - 2.0794415 * jax.random.uniform(keys[2], (4, N0, N1, N2, N3), jnp.float32) ** levels(keys[2], (4, N0, N1, N2, N3), ((1, 64), (4, 4)), -0.2, 0.2)), 0.25, 2.0),
        "cross_terms": jnp.clip(jax.random.uniform(keys[3], (6, N0, N1, N2, N3), jnp.float32, -0.3, 0.3) * levels(keys[3], (6, N0, N1, N2, N3), ((1, 64), (4, 4)), -0.4, 0.0), -0.3, 0.3),
        "flags": touch_ends((jax.random.randint(keys[4], (STEPS, N0, N1, N2, N3), 0, 3) < 1).astype(jnp.int32), jax.random.fold_in(keys[4], 1), 0, 1),
        "cotangent": centred(keys[5], (N0, N1, N2, N3), 1.0, 6.0, ((0, 64), (3, 4)), jnp.float32),
    }


asset_pairs = ((0, 1), (0, 2), (0, 3), (1, 2), (1, 3), (2, 3))

def offset_view(padded, offsets):
    return padded[tuple((slice(1 + offset, padded.shape[dimension] - 1 + offset) for dimension, offset in enumerate(offsets)))]

def unit_step(first, second, sign_first, sign_second):
    return tuple(((sign_first if dimension == first else 0) + (sign_second if dimension == second else 0) for dimension in range(4)))

def neighbours(padded, first):
    return offset_view(padded, unit_step(first, -1, 1, 0)) + offset_view(padded, unit_step(first, -1, -1, 0))

def mixed_term(padded, first, second):
    return 0.25 * (offset_view(padded, unit_step(first, second, 1, 1)) - offset_view(padded, unit_step(first, second, 1, -1)) - offset_view(padded, unit_step(first, second, -1, 1)) + offset_view(padded, unit_step(first, second, -1, -1)))

def stencil(padded, diffusion, cross_terms):
    summed = diffusion[0] * neighbours(padded, 0)
    for first in range(1, 4):
        summed = summed + diffusion[first] * neighbours(padded, first)
    for number in range(6):
        summed = summed + cross_terms[number] * mixed_term(padded, asset_pairs[number][0], asset_pairs[number][1])
    return summed

def forward(value_in, payoff, diffusion, cross_terms, flags):
    diagonal_term = 1.0 + 2.0 * lax.optimization_barrier(jnp.sum(diffusion, axis=0))
    source = value_in
    for time_step in range(STEPS):
        exercised = flags[time_step] == 1
        iterate = source
        for sweep_index in range(SWEEPS):
            padded = jnp.pad(iterate, 1)
            jacobi = (source + stencil(padded, diffusion, cross_terms)) / diagonal_term
            iterate = jnp.where(exercised, payoff, jacobi)
        source = iterate
    return source

def reference(value_in, payoff, diffusion, cross_terms, flags, cotangent):

    def wrapped(value_arg, payoff_arg, diffusion_arg, cross_arg):
        return forward(value_arg, payoff_arg, diffusion_arg, cross_arg, flags)
    result, pullback = jax.vjp(wrapped, value_in, payoff, diffusion, cross_terms)
    grads = pullback(cotangent)
    return (grads[0], grads[1], grads[2], grads[3])
```

```python
import functools
import jax
import jax.numpy as jnp
from jax import lax
from jax.experimental import pallas as pl
from jax.experimental.pallas import tpu as pltpu
from jax.sharding import PartitionSpec as P

F32 = jnp.float32
TILE = (16, 128)
BLOCK = (2, 16, 16, 128)


def lanes():
    return lax.broadcasted_iota(jnp.int32, TILE, 1)


def rows():
    return lax.broadcasted_iota(jnp.int32, TILE, 0)


def lane_roll(x, shift):
    shift = shift % 128
    return x if shift == 0 else pltpu.roll(x, shift, 1)


def up2(x, row):
    return jnp.where(row == 15, 0.0, pltpu.roll(x, 15, 0))


def down2(x, row):
    return jnp.where(row == 0, 0.0, pltpu.roll(x, 1, 0))


def wide_odd():
    return lax.rem(lax.axis_index("wide"), 2)


def narrow_odd():
    return lax.rem(lax.axis_index("narrow"), 2)


def adjoint(w_of, u_of, dif, crs, scratch, msg_a, msg_b, n1, n2, adj_of):
    q1s, p01s, p12s, p13s, x2s, y2s, x3s, y3s, q0s, p02s, p03s = scratch
    row, lane = rows(), lanes()
    zero = jnp.zeros(TILE, F32)
    for ref in (q1s, p01s, p12s, p13s):
        for r in range(2):
            ref[r, 0] = zero
            ref[r, 17] = zero
    for i in range(16):
        w = [w_of(r, i) for r in range(2)]
        h = [0.25 * w[r] for r in range(2)]
        p02 = [crs[1, r, i] * h[r] for r in range(2)]
        p03 = [crs[2, r, i] * h[r] for r in range(2)]
        for r in range(2):
            q0s[r, i] = dif[0, r, i] * w[r]
            q1s[r, i + 1] = dif[1, r, i] * w[r]
            p01s[r, i + 1] = crs[0, r, i] * h[r]
            p12s[r, i + 1] = crs[3, r, i] * h[r]
            p13s[r, i + 1] = crs[4, r, i] * h[r]
            p02s[r, i] = p02[r]
            p03s[r, i] = p03[r]
            q2 = dif[2, r, i] * w[r]
            e02 = p02[1] if r == 0 else -p02[0]
            x2s[r, i] = q2 + e02
            y2s[r, i] = q2 - e02
            q3 = dif[3, r, i] * w[r]
            p23 = crs[5, r, i] * h[r]
            e3 = (p03[1] if r == 0 else -p03[0]) + (up2(p23, row) - down2(p23, row))
            x3s[r, i] = q3 + e3
            y3s[r, i] = q3 - e3
    odd = wide_odd()
    row_a = 1 - odd
    row_b = odd
    sign_a = (2 * odd - 1).astype(F32)
    left = jnp.zeros(TILE, F32)
    right = jnp.zeros(TILE, F32)

    def put(packed, value, source, column):
        return jnp.where(lane == column, lane_roll(value, column - source), packed)

    for i in range(16):
        for r in range(2):
            u = u_of(r, i)
            left = put(left, u, 0, r * 16 + i)
            right = put(right, u, 127, r * 16 + i)
            f12 = p12s[r, i + 2] - p12s[r, i]
            f13 = p13s[r, i + 2] - p13s[r, i]
            x3 = x3s[r, i] + f13
            y3 = y3s[r, i] - f13
            x2 = x2s[r, i] + f12
            y2 = y2s[r, i] - f12
            e01 = p01s[1 - r, i + 2] - p01s[1 - r, i]
            total = q0s[1 - r, i] + q1s[r, i + 2] + q1s[r, i]
            total = total + e01 if r == 0 else total - e01
            total = total + up2(x2, row) + down2(y2, row)
            total = total + jnp.where(lane == 127, 0.0, lane_roll(x3, 127)) + jnp.where(lane == 0, 0.0, lane_roll(y3, 1))
            adj_of(r, i, total)
            left = put(left, x3, 0, 48 + r * 16 + i)
            right = put(right, y3, 127, 48 + r * 16 + i)
        p0, p1 = p03s[0, i], p03s[1, i]
        left = put(left, p0, 0, 32 + i)
        right = put(right, -p0, 127, 32 + i)
        left = put(left, -p1, 0, 80 + i)
        right = put(right, p1, 127, 80 + i)
        for msg, at, sign in ((msg_a, row_a, sign_a), (msg_b, row_b, -sign_a)):
            p02, p03 = p02s[at, i], p03s[at, i]
            d = p01s[at, i + 2] - p01s[at, i]
            d = d + up2(p02, row) - down2(p02, row)
            d = d + jnp.where(lane == 127, 0.0, lane_roll(p03, 127)) - jnp.where(lane == 0, 0.0, lane_roll(p03, 1))
            msg[1, i] = q0s[at, i] + sign * d
            msg[0, i] = u_of(at, i)
    even = narrow_odd() == 0
    n1[...] = jnp.where(even, right, left)
    n2[...] = jnp.where(even, left, right)


def stencil(fill, recv_a, recv_b, r1, r2, cor_a, cor_b, scratch, use):
    us, d2s, d3s, n2s, n3s = scratch
    row, lane = rows(), lanes()
    zero = jnp.zeros(TILE, F32)
    for r in range(4):
        for ref in (us, d2s, d3s):
            ref[r, 0] = zero
            ref[r, 17] = zero
    fill(us)
    odd = wide_odd()
    at_a, at_b = 3 * (1 - odd), 3 * odd
    us[at_a, 1:17] = recv_a[0]
    us[at_b, 1:17] = recv_b[0]
    even_n = narrow_odd() == 0
    even_w = odd == 0
    first, second = r1[...], r2[...]
    from_right = jnp.where(even_n, first, second)
    from_left = jnp.where(even_n, second, first)
    a0, a1, b0, b1 = cor_a[0], cor_a[1], cor_b[0], cor_b[1]
    a_right, a_left = jnp.where(even_n, a0, a1), jnp.where(even_n, a1, a0)
    b_right, b_left = jnp.where(even_n, b0, b1), jnp.where(even_n, b1, b0)
    low_right, low_left = jnp.where(even_w, b_right, a_right), jnp.where(even_w, b_left, a_left)
    high_right, high_left = jnp.where(even_w, a_right, b_right), jnp.where(even_w, a_left, b_left)
    packs = (
        (low_right, low_left, 16),
        (from_right, from_left, 0),
        (from_right, from_left, 16),
        (high_right, high_left, 0),
    )
    for i in range(16):
        for r in range(4):
            x = us[r, i + 1]
            pack_right, pack_left, base = packs[r]
            plus = jnp.where(lane == 127, lane_roll(pack_right, 127 - base - i), lane_roll(x, 127))
            minus = jnp.where(lane == 0, lane_roll(pack_left, -base - i), lane_roll(x, 1))
            d3s[r, i + 1] = plus - minus
            above, below = up2(x, row), down2(x, row)
            d2s[r, i + 1] = above - below
            if r in (1, 2):
                n3s[r - 1, i] = plus + minus
                n2s[r - 1, i] = above + below
    for i in range(16):
        d1 = [us[r, i + 2] - us[r, i] for r in range(4)]
        for r in range(2):
            c = r + 1
            d3 = d3s[c, i + 1]
            sums = (us[c + 1, i + 1] + us[c - 1, i + 1], us[c, i + 2] + us[c, i], n2s[r, i], n3s[r, i])
            mixed = (
                0.25 * (d1[c + 1] - d1[c - 1]),
                0.25 * (d2s[c + 1, i + 1] - d2s[c - 1, i + 1]),
                0.25 * (d3s[c + 1, i + 1] - d3s[c - 1, i + 1]),
                0.25 * (d2s[c, i + 2] - d2s[c, i]),
                0.25 * (d3s[c, i + 2] - d3s[c, i]),
                0.25 * (up2(d3, row) - down2(d3, row)),
            )
            use(r, i, sums, mixed)


def overhang(recv_a, recv_b, r1, r2, cor_a, cor_b, local, put):
    lane = lanes()
    even_w = wide_odd() == 0
    even_n = narrow_odd() == 0
    first, second = r1[...], r2[...]
    from_right = jnp.where(even_n, first, second)
    from_left = jnp.where(even_n, second, first)
    a0, a1, b0, b1 = cor_a[0], cor_a[1], cor_b[0], cor_b[1]
    a_right, a_left = jnp.where(even_n, a0, a1), jnp.where(even_n, a1, a0)
    b_right, b_left = jnp.where(even_n, b0, b1), jnp.where(even_n, b1, b0)
    low_right, low_left = jnp.where(even_w, b_right, a_right), jnp.where(even_w, b_left, a_left)
    high_right, high_left = jnp.where(even_w, a_right, b_right), jnp.where(even_w, a_left, b_left)

    def gathered(own, low, high):
        return lane_roll(own, -48) + jnp.where(lane < 16, lane_roll(low, -80), lane_roll(high, -16))

    cols_right = gathered(from_right, low_right, high_right)
    cols_left = gathered(from_left, low_left, high_left)
    odd = wide_odd()
    for i in range(16):
        for r in range(2):
            wide = jnp.where(even_w, recv_b[1, i], recv_a[1, i]) if r == 0 else jnp.where(even_w, recv_a[1, i], recv_b[1, i])
            at = r * 16 + i
            column = jnp.where(lane == 127, lane_roll(cols_right, 127 - at), jnp.where(lane == 0, lane_roll(cols_left, -at), 0.0))
            put(r, i, local(r, i) + wide + column)


ADJOINT_SCRATCH = [pltpu.VMEM((2, 18, *TILE), F32)] * 4 + [pltpu.VMEM(BLOCK, F32)] * 7
STENCIL_SCRATCH = [pltpu.VMEM((4, 18, *TILE), F32)] * 3 + [pltpu.VMEM(BLOCK, F32)] * 2


def kernel_a(cot, flg, dif, crs, val, msg_a, msg_b, n1, n2, inv, w2, adj, *scratch):
    def weight(r, i):
        recip = 1.0 / (1.0 + 2.0 * (dif[0, r, i] + dif[1, r, i] + dif[2, r, i] + dif[3, r, i]))
        inv[r, i] = recip
        w = jnp.where(flg[r, i] == 1, 0.0, cot[r, i] * recip)
        w2[r, i] = w
        return w

    def keep(r, i, total):
        adj[r, i] = total

    adjoint(weight, lambda r, i: val[r, i], dif, crs, scratch, msg_a, msg_b, n1, n2, keep)


def kernel_b(val, pay, flg, dif, crs, inv, adj_in, ra, rb, r1, r2, ca, cb, msg_a, msg_b, n1, n2, u1, w1, adj1, adj0, *scratch):
    def fill(us):
        us[1:3, 1:17] = val[...]

    def use(r, i, sums, mixed):
        total = val[r, i]
        for k in range(4):
            total = total + dif[k, r, i] * sums[k]
        for k in range(6):
            total = total + crs[k, r, i] * mixed[k]
        u1[r, i] = jnp.where(flg[r, i] == 1, pay[r, i], total * inv[r, i])

    stencil(fill, ra, rb, r1, r2, ca, cb, scratch[:5], use)

    def put(r, i, total):
        adj1[r, i] = total
        w1[r, i] = jnp.where(flg[r, i] == 1, 0.0, total * inv[r, i])

    overhang(ra, rb, r1, r2, ca, cb, lambda r, i: adj_in[r, i], put)

    def keep(r, i, total):
        adj0[r, i] = total

    adjoint(lambda r, i: w1[r, i], lambda r, i: u1[r, i], dif, crs, scratch[5:], msg_a, msg_b, n1, n2, keep)


def kernel_m(val, flg, dif, crs, inv, w1, w2, cot, adj1, adj0, ra, rb, r1, r2, ca, cb, gpay, part, gd, gc, *scratch):
    def fill(us):
        us[1:3, 1:17] = val[...]

    def use(r, i, sums, mixed):
        total = val[r, i]
        for k in range(4):
            total = total + dif[k, r, i] * sums[k]
        for k in range(6):
            total = total + crs[k, r, i] * mixed[k]
        twice = 2.0 * (total * inv[r, i])
        w = w1[r, i]
        for k in range(4):
            gd[k, r, i] = w * (sums[k] - twice)
        for k in range(6):
            gc[k, r, i] = w * mixed[k]
        gpay[r, i] = jnp.where(flg[r, i] == 1, cot[r, i] + adj1[r, i], 0.0)
        part[r, i] = adj0[r, i] + w + w2[r, i]

    stencil(fill, ra, rb, r1, r2, ca, cb, scratch, use)


def kernel_c(val, u1, dif, crs, inv, w2, part, pd, pc, ra, rb, r1, r2, ca, cb, gval, gd, gc, *scratch):
    def fill(us):
        us[1:3, 1:17] = u1[...]

    def use(r, i, sums, mixed):
        total = val[r, i]
        for k in range(4):
            total = total + dif[k, r, i] * sums[k]
        for k in range(6):
            total = total + crs[k, r, i] * mixed[k]
        twice = 2.0 * (total * inv[r, i])
        w = w2[r, i]
        for k in range(4):
            gd[k, r, i] = pd[k, r, i] + w * (sums[k] - twice)
        for k in range(6):
            gc[k, r, i] = pc[k, r, i] + w * mixed[k]

    stencil(fill, ra, rb, r1, r2, ca, cb, scratch, use)

    def put(r, i, total):
        gval[r, i] = total

    overhang(ra, rb, r1, r2, ca, cb, lambda r, i: part[r, i], put)


def call(kernel, outs, scratch, flops, *args):
    return pl.pallas_call(
        kernel,
        out_shape=[jax.ShapeDtypeStruct(shape, F32) for shape in outs],
        in_specs=[pl.BlockSpec(memory_space=pltpu.VMEM)] * len(args),
        out_specs=[pl.BlockSpec(memory_space=pltpu.VMEM)] * len(outs),
        scratch_shapes=scratch,
        cost_estimate=pl.CostEstimate(flops=flops, bytes_accessed=4 << 20, transcendentals=0),
        compiler_params=pltpu.CompilerParams(vmem_limit_bytes=40 << 20),
    )(*args)


def swap(x, axis, odd, count):
    pairs = []
    for i in range(odd, count - 1, 2):
        pairs += [(i, i + 1), (i + 1, i)]
    return lax.ppermute(x, axis, pairs)


def exchange(msg_a, msg_b, n1, n2):
    wide, narrow = lax.axis_size("wide"), lax.axis_size("narrow")
    rb = swap(msg_b, "wide", 1, wide)
    ra = swap(msg_a, "wide", 0, wide)
    r1 = swap(n1, "narrow", 0, narrow)
    r2 = swap(n2, "narrow", 1, narrow)
    corners = jnp.stack([r1, r2])
    cb = swap(corners, "wide", 1, wide)
    ca = swap(corners, "wide", 0, wide)
    return ra, rb, r1, r2, ca, cb


def body(value_in, payoff, diffusion, cross_terms, flags, cotangent):
    flg = flags[0]
    message = (2, 16, *TILE)
    sends = [message, message, TILE, TILE]
    msg_a, msg_b, n1, n2, inv, w2, adj = call(
        kernel_a, sends + [BLOCK] * 3, ADJOINT_SCRATCH, 40 << 16, cotangent, flg, diffusion, cross_terms, value_in
    )
    first = exchange(msg_a, msg_b, n1, n2)
    msg_a, msg_b, n1, n2, u1, w1, adj1, adj0 = call(
        kernel_b, sends + [BLOCK] * 4, STENCIL_SCRATCH + ADJOINT_SCRATCH, 80 << 16, value_in, payoff, flg, diffusion, cross_terms, inv, adj, *first
    )
    second = exchange(msg_a, msg_b, n1, n2)
    gpay, part, pd, pc = call(
        kernel_m, [BLOCK, BLOCK, (4, *BLOCK), (6, *BLOCK)], STENCIL_SCRATCH, 60 << 16,
        value_in, flg, diffusion, cross_terms, inv, w1, w2, cotangent, adj1, adj0, *first,
    )
    gval, gd, gc = call(
        kernel_c, [BLOCK, (4, *BLOCK), (6, *BLOCK)], STENCIL_SCRATCH, 60 << 16,
        value_in, u1, diffusion, cross_terms, inv, w2, part, pd, pc, *second,
    )
    return gval, gpay, gd, gc


def solution(mesh):
    field = P("wide", None, None, "narrow")
    stack = P(None, "wide", None, None, "narrow")
    return jax.shard_map(
        body, mesh=mesh, in_specs=(field, field, stack, stack, stack, field), out_specs=(field, field, stack, stack), check_vma=False
    )
```

```python
import jax
import jax.numpy as jnp
from jax import lax
from jax.experimental import pallas as pl
from jax.experimental.pallas import tpu as pltpu
from jax.sharding import PartitionSpec as P

F32 = jnp.float32
TILE = (16, 128)
BLOCK = (2, 16, 16, 128)
CHUNK = 4
CHUNKS = 16 // CHUNK


def lanes():
    return lax.broadcasted_iota(jnp.int32, TILE, 1)


def rows():
    return lax.broadcasted_iota(jnp.int32, TILE, 0)


def lane_roll(x, shift):
    shift = shift % 128
    return x if shift == 0 else pltpu.roll(x, shift, 1)


def up2(x, row):
    return jnp.where(row == 15, 0.0, pltpu.roll(x, 15, 0))


def down2(x, row):
    return jnp.where(row == 0, 0.0, pltpu.roll(x, 1, 0))


def both(ref, r, i):
    if i == 0:
        return ref[r, 1], ref[r, 1]
    if i == 15:
        return ref[r, 14], -ref[r, 14]
    return ref[r, i + 1] + ref[r, i - 1], ref[r, i + 1] - ref[r, i - 1]


def wide_odd():
    return lax.rem(lax.axis_index("wide"), 2)


def narrow_odd():
    return lax.rem(lax.axis_index("narrow"), 2)


def narrow_sides(first, second):
    even = narrow_odd() == 0
    return jnp.where(even, first, second), jnp.where(even, second, first)


def corner_sides(cor_a, cor_b):
    even = wide_odd() == 0
    a_right, a_left = narrow_sides(cor_a[0], cor_a[1])
    b_right, b_left = narrow_sides(cor_b[0], cor_b[1])
    low = jnp.where(even, b_right, a_right), jnp.where(even, b_left, a_left)
    high = jnp.where(even, a_right, b_right), jnp.where(even, a_left, b_left)
    return low, high


def from_wide(ra, rb, part, r, i):
    even = wide_odd() == 0
    low, high = (rb, ra) if r == 0 else (ra, rb)
    return jnp.where(even, low[part, i], high[part, i])


def adjoint(w_of, u_of, dif, crs, scratch, msg_a, msg_b, n1, n2, adj_of):
    q1s, p01s, p12s, p13s, x2s, y2s, x3s, y3s, q0s, p02s, p03s = scratch
    row, lane = rows(), lanes()
    for i in range(16):
        w = [w_of(r, i) for r in range(2)]
        h = [0.25 * w[r] for r in range(2)]
        p02 = [crs[1, r, i] * h[r] for r in range(2)]
        p03 = [crs[2, r, i] * h[r] for r in range(2)]
        for r in range(2):
            q0s[r, i] = dif[0, r, i] * w[r]
            q1s[r, i] = dif[1, r, i] * w[r]
            p01s[r, i] = crs[0, r, i] * h[r]
            p12s[r, i] = crs[3, r, i] * h[r]
            p13s[r, i] = crs[4, r, i] * h[r]
            p02s[r, i] = p02[r]
            p03s[r, i] = p03[r]
            q2 = dif[2, r, i] * w[r]
            e02 = p02[1] if r == 0 else -p02[0]
            x2s[r, i] = q2 + e02
            y2s[r, i] = q2 - e02
            q3 = dif[3, r, i] * w[r]
            p23 = crs[5, r, i] * h[r]
            e3 = (p03[1] if r == 0 else -p03[0]) + (up2(p23, row) - down2(p23, row))
            x3s[r, i] = q3 + e3
            y3s[r, i] = q3 - e3
    odd = wide_odd()
    row_a = 1 - odd
    row_b = odd
    sign_a = (2 * odd - 1).astype(F32)
    left = jnp.zeros(TILE, F32)
    right = jnp.zeros(TILE, F32)

    def put(packed, value, source, column):
        return jnp.where(lane == column, lane_roll(value, column - source), packed)

    for i in range(16):
        for r in range(2):
            u = u_of(r, i)
            left = put(left, u, 0, r * 16 + i)
            right = put(right, u, 127, r * 16 + i)
            f12 = both(p12s, r, i)[1]
            f13 = both(p13s, r, i)[1]
            x3 = x3s[r, i] + f13
            y3 = y3s[r, i] - f13
            x2 = x2s[r, i] + f12
            y2 = y2s[r, i] - f12
            e01 = both(p01s, 1 - r, i)[1]
            total = q0s[1 - r, i] + both(q1s, r, i)[0]
            total = total + e01 if r == 0 else total - e01
            total = total + up2(x2, row) + down2(y2, row)
            total = total + jnp.where(lane == 127, 0.0, lane_roll(x3, 127)) + jnp.where(lane == 0, 0.0, lane_roll(y3, 1))
            adj_of(r, i, total)
            left = put(left, x3, 0, 48 + r * 16 + i)
            right = put(right, y3, 127, 48 + r * 16 + i)
        p0, p1 = p03s[0, i], p03s[1, i]
        left = put(left, p0, 0, 32 + i)
        right = put(right, -p0, 127, 32 + i)
        left = put(left, -p1, 0, 80 + i)
        right = put(right, p1, 127, 80 + i)
        for msg, at, sign in ((msg_a, row_a, sign_a), (msg_b, row_b, -sign_a)):
            p02, p03 = p02s[at, i], p03s[at, i]
            d = both(p01s, at, i)[1]
            d = d + up2(p02, row) - down2(p02, row)
            d = d + jnp.where(lane == 127, 0.0, lane_roll(p03, 127)) - jnp.where(lane == 0, 0.0, lane_roll(p03, 1))
            msg[1, i] = q0s[at, i] + sign * d
            msg[0, i] = u_of(at, i)
    even = narrow_odd() == 0
    n1[...] = jnp.where(even, right, left)
    n2[...] = jnp.where(even, left, right)


def inner(us, r1, r2, scratch):
    d2s, d3s, n2s, n3s = scratch
    row, lane = rows(), lanes()
    from_right, from_left = narrow_sides(r1[...], r2[...])
    for i in range(16):
        for r in range(2):
            x = us[r, i]
            at = r * 16 + i
            plus = jnp.where(lane == 127, lane_roll(from_right, 127 - at), lane_roll(x, 127))
            minus = jnp.where(lane == 0, lane_roll(from_left, -at), lane_roll(x, 1))
            above, below = up2(x, row), down2(x, row)
            d3s[r, i] = plus - minus
            d2s[r, i] = above - below
            n3s[r, i] = plus + minus
            n2s[r, i] = above + below

    def at(r, i):
        d3 = d3s[r, i]
        sign = 0.25 if r == 0 else -0.25
        sums = (us[1 - r, i], both(us, r, i)[0], n2s[r, i], n3s[r, i])
        mixed = (
            sign * both(us, 1 - r, i)[1],
            sign * d2s[1 - r, i],
            sign * d3s[1 - r, i],
            0.25 * both(d2s, r, i)[1],
            0.25 * both(d3s, r, i)[1],
            0.25 * (up2(d3, row) - down2(d3, row)),
        )
        return sums, mixed

    return at


def outer(ra, rb, ca, cb):
    row, lane = rows(), lanes()
    low, high = corner_sides(ca, cb)

    def at(r, i):
        x = from_wide(ra, rb, 0, r, i)
        (pack_right, pack_left), base = (low, 16) if r == 0 else (high, 0)
        sign = -0.25 if r == 0 else 0.25
        if i == 0:
            d1 = from_wide(ra, rb, 0, r, 1)
        elif i == 15:
            d1 = -from_wide(ra, rb, 0, r, 14)
        else:
            d1 = from_wide(ra, rb, 0, r, i + 1) - from_wide(ra, rb, 0, r, i - 1)
        d2 = up2(x, row) - down2(x, row)
        plus = jnp.where(lane == 127, lane_roll(pack_right, 127 - base - i), lane_roll(x, 127))
        minus = jnp.where(lane == 0, lane_roll(pack_left, -base - i), lane_roll(x, 1))
        return x, (sign * d1, sign * d2, sign * (plus - minus))

    return at


def columns(right, left):
    lane = lanes()

    def at(r, i):
        k = r * 16 + i
        return jnp.where(lane == 127, lane_roll(right, 127 - k), jnp.where(lane == 0, lane_roll(left, -k), 0.0))

    return at


def narrow_overhang(r1, r2):
    right, left = narrow_sides(r1[...], r2[...])
    return columns(lane_roll(right, -48), lane_roll(left, -48))


def corner_overhang(ca, cb):
    lane = lanes()
    low, high = corner_sides(ca, cb)
    merged = [jnp.where(lane < 16, lane_roll(low[k], -80), lane_roll(high[k], -16)) for k in range(2)]
    return columns(*merged)


ADJOINT_SCRATCH = [pltpu.VMEM(BLOCK, F32)] * 11
INNER_SCRATCH = [pltpu.VMEM(BLOCK, F32)] * 4


def kernel_a(cot_h, flg_h, dif_h, crs_h, val_h, msg_a, msg_b, n1, n2, inv, w2, adj, cot, flg, val, dif, crs, sems, *scratch):
    copies = []
    for c in range(CHUNKS):
        span = pl.ds(c * CHUNK, CHUNK)
        group = []
        for k, (src, dst) in enumerate(((cot_h, cot), (flg_h, flg), (val_h, val))):
            group.append(pltpu.make_async_copy(src.at[:, span], dst.at[:, span], sems.at[c, k]))
        for k, (src, dst) in enumerate(((dif_h, dif), (crs_h, crs))):
            group.append(pltpu.make_async_copy(src.at[:, :, span], dst.at[:, :, span], sems.at[c, 3 + k]))
        for copy in group:
            copy.start()
        copies.append(group)

    def weight(r, i):
        if r == 0 and i % CHUNK == 0:
            for copy in copies[i // CHUNK]:
                copy.wait()
        recip = 1.0 / (1.0 + 2.0 * (dif[0, r, i] + dif[1, r, i] + dif[2, r, i] + dif[3, r, i]))
        inv[r, i] = recip
        w = jnp.where(flg[r, i] == 1, 0.0, cot[r, i] * recip)
        w2[r, i] = w
        return w

    def keep(r, i, total):
        adj[r, i] = total

    adjoint(weight, lambda r, i: val[r, i], dif, crs, scratch, msg_a, msg_b, n1, n2, keep)


def kernel_p(val, dif, crs, adj_in, r1, r2, total, adj, *scratch):
    at = inner(val, r1, r2, scratch)
    column = narrow_overhang(r1, r2)
    for i in range(16):
        for r in range(2):
            sums, mixed = at(r, i)
            value = val[r, i]
            for k in range(4):
                value = value + dif[k, r, i] * sums[k]
            for k in range(6):
                value = value + crs[k, r, i] * mixed[k]
            total[r, i] = value
            adj[r, i] = adj_in[r, i] + column(r, i)


def kernel_b(pay, flg, dif, crs, inv, total, adj_in, ra, rb, ca, cb, msg_a, msg_b, n1, n2, u1, w1, adj1, adj0, *scratch):
    beyond = outer(ra, rb, ca, cb)
    column = corner_overhang(ca, cb)

    def weight(r, i):
        x, mixed = beyond(r, i)
        value = total[r, i] + dif[0, r, i] * x
        for k in range(3):
            value = value + crs[k, r, i] * mixed[k]
        exercised = flg[r, i] == 1
        recip = inv[r, i]
        u1[r, i] = jnp.where(exercised, pay[r, i], value * recip)
        adjoint_value = adj_in[r, i] + from_wide(ra, rb, 1, r, i) + column(r, i)
        adj1[r, i] = adjoint_value
        w = jnp.where(exercised, 0.0, adjoint_value * recip)
        w1[r, i] = w
        return w

    def keep(r, i, value):
        adj0[r, i] = value

    adjoint(weight, lambda r, i: u1[r, i], dif, crs, scratch, msg_a, msg_b, n1, n2, keep)


def kernel_m(
    val, u1, flg, dif, crs, inv, total, w1, w2, cot, adj1, adj0, ra, rb, r1, r2, ca, cb, s1, s2,
    gpay, gc, part, pd, pc, out_pay, out_gc, sems, *scratch,
):
    first = inner(val, r1, r2, scratch[:4])
    beyond = outer(ra, rb, ca, cb)
    second = inner(u1, s1, s2, scratch[4:])
    column = narrow_overhang(s1, s2)
    for i in range(16):
        for r in range(2):
            sums, mixed = first(r, i)
            x, more = beyond(r, i)
            sums = (sums[0] + x, *sums[1:])
            value = total[r, i] + dif[0, r, i] * x
            for k in range(3):
                value = value + crs[k, r, i] * more[k]
            mixed = (*(mixed[k] + more[k] for k in range(3)), *mixed[3:])
            sums_2, mixed_2 = second(r, i)
            value_2 = val[r, i]
            for k in range(4):
                value_2 = value_2 + dif[k, r, i] * sums_2[k]
            for k in range(6):
                value_2 = value_2 + crs[k, r, i] * mixed_2[k]
            recip = 2.0 * inv[r, i]
            twice, twice_2 = value * recip, value_2 * recip
            w, v = w1[r, i], w2[r, i]
            for k in range(4):
                pd[k, r, i] = w * (sums[k] - twice) + v * (sums_2[k] - twice_2)
            for k in range(3):
                pc[k, r, i] = w * mixed[k] + v * mixed_2[k]
            for k in range(3, 6):
                out_gc[k - 3, r, i] = w * mixed[k] + v * mixed_2[k]
            out_pay[r, i] = jnp.where(flg[r, i] == 1, cot[r, i] + adj1[r, i], 0.0)
            part[r, i] = adj0[r, i] + w + v + column(r, i)
    copies = [pltpu.make_async_copy(out_pay, gpay, sems.at[0]), pltpu.make_async_copy(out_gc, gc.at[pl.ds(3, 3)], sems.at[1])]
    for copy in copies:
        copy.start()
    for copy in copies:
        copy.wait()


def kernel_c(dif, crs, inv, w2, part, pd, pc, ra, rb, ca, cb, gc_in, gval, gd, gc, out_val, out_d, out_c, sems):
    del gc_in
    beyond = outer(ra, rb, ca, cb)
    column = corner_overhang(ca, cb)
    copies = []
    for i in range(16):
        for r in range(2):
            x, more = beyond(r, i)
            value = dif[0, r, i] * x
            for k in range(3):
                value = value + crs[k, r, i] * more[k]
            v = w2[r, i]
            change = (2.0 * inv[r, i]) * v * value
            out_d[0, r, i] = pd[0, r, i] + (v * x - change)
            for k in range(1, 4):
                out_d[k, r, i] = pd[k, r, i] - change
            for k in range(3):
                out_c[k, r, i] = pc[k, r, i] + v * more[k]
            out_val[r, i] = part[r, i] + from_wide(ra, rb, 1, r, i) + column(r, i)
        if i % CHUNK == CHUNK - 1:
            c = i // CHUNK
            span = pl.ds(c * CHUNK, CHUNK)
            group = [
                pltpu.make_async_copy(out_d.at[:, :, span], gd.at[:, :, span], sems.at[c, 0]),
                pltpu.make_async_copy(out_c.at[:, :, span], gc.at[pl.ds(0, 3), :, span], sems.at[c, 1]),
                pltpu.make_async_copy(out_val.at[:, span], gval.at[:, span], sems.at[c, 2]),
            ]
            for copy in group:
                copy.start()
            copies += group
    for copy in copies:
        copy.wait()


V = pltpu.VMEM
H = pltpu.HBM


def call(kernel, outs, scratch, flops, args, spaces=None, aliases=None, limit=160):
    return pl.pallas_call(
        kernel,
        out_shape=[jax.ShapeDtypeStruct(out[0], out[2] if len(out) > 2 else F32) for out in outs],
        in_specs=[pl.BlockSpec(memory_space=space) for space in (spaces or [V] * len(args))],
        out_specs=[pl.BlockSpec(memory_space=out[1]) for out in outs],
        scratch_shapes=scratch,
        input_output_aliases=aliases or {},
        cost_estimate=pl.CostEstimate(flops=flops, bytes_accessed=4 << 20, transcendentals=0),
        compiler_params=pltpu.CompilerParams(vmem_limit_bytes=limit << 18),
    )(*args)


def swap(x, axis, odd):
    pairs = []
    for i in range(odd, lax.axis_size(axis) - 1, 2):
        pairs += [(i, i + 1), (i + 1, i)]
    return lax.ppermute(x, axis, pairs)


def exchange(msg_a, msg_b, n1, n2):
    r2 = swap(n2, "narrow", 1)
    rb = swap(msg_b, "wide", 1)
    r1 = swap(n1, "narrow", 0)
    ra = swap(msg_a, "wide", 0)
    corners = jnp.stack([r1, r2])
    cb = swap(corners, "wide", 1)
    ca = swap(corners, "wide", 0)
    return ra, rb, r1, r2, ca, cb


def body(value_in, payoff, diffusion, cross_terms, flags, cotangent):
    four, six = (4, *BLOCK), (6, *BLOCK)
    message = (2, 16, *TILE)
    sends = [(message, V), (message, V), (TILE, V), (TILE, V)]
    block = (BLOCK, V)
    msg_a, msg_b, n1, n2, inv, w2, adj, cot, flg, val = call(
        kernel_a,
        [*sends, block, block, block, block, (BLOCK, V, jnp.int32), block],
        [pltpu.VMEM(four, F32), pltpu.VMEM(six, F32), pltpu.SemaphoreType.DMA((CHUNKS, 5)), *ADJOINT_SCRATCH],
        40 << 16,
        (cotangent, flags[0], diffusion, cross_terms, value_in),
        [H] * 5,
        limit=207,
    )
    ra, rb, r1, r2, ca, cb = exchange(msg_a, msg_b, n1, n2)
    total, adj = call(kernel_p, [block, block], INNER_SCRATCH, 40 << 16, (val, diffusion, cross_terms, adj, r1, r2))
    msg_a, msg_b, n1, n2, u1, w1, adj1, adj0 = call(
        kernel_b,
        [*sends, block, block, block, block],
        ADJOINT_SCRATCH,
        60 << 16,
        (payoff, flg, diffusion, cross_terms, inv, total, adj, ra, rb, ca, cb),
    )
    sa, sb, s1, s2, da, db = exchange(msg_a, msg_b, n1, n2)
    gpay, gc, part, pd, pc = call(
        kernel_m,
        [(BLOCK, H), (six, H), block, (four, V), ((3, *BLOCK), V)],
        [pltpu.VMEM(BLOCK, F32), pltpu.VMEM((3, *BLOCK), F32), pltpu.SemaphoreType.DMA((2,)), *INNER_SCRATCH, *INNER_SCRATCH],
        120 << 16,
        (val, u1, flg, diffusion, cross_terms, inv, total, w1, w2, cot, adj1, adj0, ra, rb, r1, r2, ca, cb, s1, s2),
    )
    gval, gd, gc = call(
        kernel_c,
        [(BLOCK, H), (four, H), (six, H)],
        [pltpu.VMEM(BLOCK, F32), pltpu.VMEM(four, F32), pltpu.VMEM((3, *BLOCK), F32), pltpu.SemaphoreType.DMA((CHUNKS, 3))],
        40 << 16,
        (diffusion, cross_terms, inv, w2, part, pd, pc, sa, sb, da, db, gc),
        [V] * 11 + [H],
        {11: 2},
    )
    return gval, gpay, gd, gc


def solution(mesh):
    field = P("wide", None, None, "narrow")
    stack = P(None, "wide", None, None, "narrow")
    return jax.shard_map(
        body, mesh=mesh, in_specs=(field, field, stack, stack, stack, field), out_specs=(field, field, stack, stack), check_vma=False
    )
```

```python
import functools

import jax
import jax.numpy as jnp
from jax import lax
from jax.experimental import pallas as pl
from jax.experimental.pallas import tpu as pltpu
from jax.sharding import PartitionSpec as P

F32 = jnp.float32
TILE = (16, 128)
BLOCK = (2, 16, 16, 128)
OUT_CHUNK = 8
IN_CHUNK = 8


def lanes():
    return lax.broadcasted_iota(jnp.int32, TILE, 1)


def rows():
    return lax.broadcasted_iota(jnp.int32, TILE, 0)


def lane_roll(x, shift):
    shift = shift % 128
    return x if shift == 0 else pltpu.roll(x, shift, 1)


def up2(x, row):
    return jnp.where(row == 15, 0.0, pltpu.roll(x, 15, 0))


def down2(x, row):
    return jnp.where(row == 0, 0.0, pltpu.roll(x, 1, 0))


def both(ref, r, i):
    if i == 0:
        return ref[r, 1], ref[r, 1]
    if i == 15:
        return ref[r, 14], -ref[r, 14]
    return ref[r, i + 1] + ref[r, i - 1], ref[r, i + 1] - ref[r, i - 1]


def wide_odd():
    return lax.rem(lax.axis_index("wide"), 2)


def narrow_odd():
    return lax.rem(lax.axis_index("narrow"), 2)


def narrow_sides(first, second):
    even = narrow_odd() == 0
    return jnp.where(even, first, second), jnp.where(even, second, first)


def corner_sides(cor_a, cor_b):
    even = wide_odd() == 0
    a_right, a_left = narrow_sides(cor_a[0], cor_a[1])
    b_right, b_left = narrow_sides(cor_b[0], cor_b[1])
    low = jnp.where(even, b_right, a_right), jnp.where(even, b_left, a_left)
    high = jnp.where(even, a_right, b_right), jnp.where(even, a_left, b_left)
    return low, high


def from_wide(ra, rb, part, r, i):
    even = wide_odd() == 0
    low, high = (rb, ra) if r == 0 else (ra, rb)
    return jnp.where(even, low[part, i], high[part, i])


def adjoint(w_of, u_of, dif, crs, scratch, msg_a, msg_b, n1, n2, adj_of):
    q1s, p01s, p12s, p13s, x2s, y2s, x3s, y3s, q0s, p02s, p03s = scratch
    row, lane = rows(), lanes()
    for i in range(16):
        w = [w_of(r, i) for r in range(2)]
        h = [0.25 * w[r] for r in range(2)]
        p02 = [crs[1, r, i] * h[r] for r in range(2)]
        p03 = [crs[2, r, i] * h[r] for r in range(2)]
        for r in range(2):
            q0s[r, i] = dif[0, r, i] * w[r]
            q1s[r, i] = dif[1, r, i] * w[r]
            p01s[r, i] = crs[0, r, i] * h[r]
            p12s[r, i] = crs[3, r, i] * h[r]
            p13s[r, i] = crs[4, r, i] * h[r]
            p02s[r, i] = p02[r]
            p03s[r, i] = p03[r]
            q2 = dif[2, r, i] * w[r]
            e02 = p02[1] if r == 0 else -p02[0]
            x2s[r, i] = q2 + e02
            y2s[r, i] = q2 - e02
            q3 = dif[3, r, i] * w[r]
            p23 = crs[5, r, i] * h[r]
            e3 = (p03[1] if r == 0 else -p03[0]) + (up2(p23, row) - down2(p23, row))
            x3s[r, i] = q3 + e3
            y3s[r, i] = q3 - e3
    odd = wide_odd()
    row_a = 1 - odd
    row_b = odd
    sign_a = (2 * odd - 1).astype(F32)
    left = jnp.zeros(TILE, F32)
    right = jnp.zeros(TILE, F32)

    def put(packed, value, source, column):
        return jnp.where(lane == column, lane_roll(value, column - source), packed)

    for i in range(16):
        for r in range(2):
            u = u_of(r, i)
            left = put(left, u, 0, r * 16 + i)
            right = put(right, u, 127, r * 16 + i)
            f12 = both(p12s, r, i)[1]
            f13 = both(p13s, r, i)[1]
            x3 = x3s[r, i] + f13
            y3 = y3s[r, i] - f13
            x2 = x2s[r, i] + f12
            y2 = y2s[r, i] - f12
            e01 = both(p01s, 1 - r, i)[1]
            total = q0s[1 - r, i] + both(q1s, r, i)[0]
            total = total + e01 if r == 0 else total - e01
            total = total + up2(x2, row) + down2(y2, row)
            total = total + jnp.where(lane == 127, 0.0, lane_roll(x3, 127)) + jnp.where(lane == 0, 0.0, lane_roll(y3, 1))
            adj_of(r, i, total)
            left = put(left, x3, 0, 48 + r * 16 + i)
            right = put(right, y3, 127, 48 + r * 16 + i)
        p0, p1 = p03s[0, i], p03s[1, i]
        left = put(left, p0, 0, 32 + i)
        right = put(right, -p0, 127, 32 + i)
        left = put(left, -p1, 0, 80 + i)
        right = put(right, p1, 127, 80 + i)
        for msg, at, sign in ((msg_a, row_a, sign_a), (msg_b, row_b, -sign_a)):
            p02, p03 = p02s[at, i], p03s[at, i]
            d = both(p01s, at, i)[1]
            d = d + up2(p02, row) - down2(p02, row)
            d = d + jnp.where(lane == 127, 0.0, lane_roll(p03, 127)) - jnp.where(lane == 0, 0.0, lane_roll(p03, 1))
            msg[1, i] = q0s[at, i] + sign * d
            msg[0, i] = u_of(at, i)
    even = narrow_odd() == 0
    n1[...] = jnp.where(even, right, left)
    n2[...] = jnp.where(even, left, right)


def inner(us, r1, r2, scratch):
    d2s, d3s, n2s, n3s = scratch
    row, lane = rows(), lanes()
    from_right, from_left = narrow_sides(r1[...], r2[...])
    for i in range(16):
        for r in range(2):
            x = us[r, i]
            at = r * 16 + i
            plus = jnp.where(lane == 127, lane_roll(from_right, 127 - at), lane_roll(x, 127))
            minus = jnp.where(lane == 0, lane_roll(from_left, -at), lane_roll(x, 1))
            above, below = up2(x, row), down2(x, row)
            d3s[r, i] = plus - minus
            d2s[r, i] = above - below
            n3s[r, i] = plus + minus
            n2s[r, i] = above + below

    def at(r, i):
        d3 = d3s[r, i]
        sign = 0.25 if r == 0 else -0.25
        sums = (us[1 - r, i], both(us, r, i)[0], n2s[r, i], n3s[r, i])
        mixed = (
            sign * both(us, 1 - r, i)[1],
            sign * d2s[1 - r, i],
            sign * d3s[1 - r, i],
            0.25 * both(d2s, r, i)[1],
            0.25 * both(d3s, r, i)[1],
            0.25 * (up2(d3, row) - down2(d3, row)),
        )
        return sums, mixed

    return at


def outer(ra, rb, ca, cb):
    row, lane = rows(), lanes()
    low, high = corner_sides(ca, cb)

    def at(r, i):
        x = from_wide(ra, rb, 0, r, i)
        (pack_right, pack_left), base = (low, 16) if r == 0 else (high, 0)
        sign = -0.25 if r == 0 else 0.25
        if i == 0:
            d1 = from_wide(ra, rb, 0, r, 1)
        elif i == 15:
            d1 = -from_wide(ra, rb, 0, r, 14)
        else:
            d1 = from_wide(ra, rb, 0, r, i + 1) - from_wide(ra, rb, 0, r, i - 1)
        d2 = up2(x, row) - down2(x, row)
        plus = jnp.where(lane == 127, lane_roll(pack_right, 127 - base - i), lane_roll(x, 127))
        minus = jnp.where(lane == 0, lane_roll(pack_left, -base - i), lane_roll(x, 1))
        return x, (sign * d1, sign * d2, sign * (plus - minus))

    return at


def columns(right, left):
    lane = lanes()

    def at(r, i):
        k = r * 16 + i
        return jnp.where(lane == 127, lane_roll(right, 127 - k), jnp.where(lane == 0, lane_roll(left, -k), 0.0))

    return at


def narrow_overhang(r1, r2):
    right, left = narrow_sides(r1[...], r2[...])
    return columns(lane_roll(right, -48), lane_roll(left, -48))


def corner_overhang(ca, cb):
    lane = lanes()
    low, high = corner_sides(ca, cb)
    merged = [jnp.where(lane < 16, lane_roll(low[k], -80), lane_roll(high[k], -16)) for k in range(2)]
    return columns(*merged)


ADJOINT_SCRATCH = [pltpu.VMEM(BLOCK, F32)] * 11
INNER_SCRATCH = [pltpu.VMEM(BLOCK, F32)] * 4


def kernel_a(cot_h, flg_h, dif_h, crs_h, val_h, msg_a, msg_b, n1, n2, inv, w2, adj, cot, flg, val, dif, crs, sems, *scratch):
    copies = []
    for c in range(16 // IN_CHUNK):
        span = pl.ds(c * IN_CHUNK, IN_CHUNK)
        group = []
        for k, (src, dst) in enumerate(((cot_h, cot), (flg_h, flg), (val_h, val))):
            group.append(pltpu.make_async_copy(src.at[:, span], dst.at[:, span], sems.at[c, k]))
        for k, (src, dst) in enumerate(((dif_h, dif), (crs_h, crs))):
            group.append(pltpu.make_async_copy(src.at[:, :, span], dst.at[:, :, span], sems.at[c, 3 + k]))
        for copy in group:
            copy.start()
        copies.append(group)

    def weight(r, i):
        if r == 0 and i % IN_CHUNK == 0:
            for copy in copies[i // IN_CHUNK]:
                copy.wait()
        recip = 1.0 / (1.0 + 2.0 * (dif[0, r, i] + dif[1, r, i] + dif[2, r, i] + dif[3, r, i]))
        inv[r, i] = recip
        w = jnp.where(flg[r, i] == 1, 0.0, cot[r, i] * recip)
        w2[r, i] = w
        return w

    def keep(r, i, total):
        adj[r, i] = total

    adjoint(weight, lambda r, i: val[r, i], dif, crs, scratch, msg_a, msg_b, n1, n2, keep)


def kernel_p(val, dif, crs, adj_in, r1, r2, total, adj, *scratch):
    at = inner(val, r1, r2, scratch)
    column = narrow_overhang(r1, r2)
    for i in range(16):
        for r in range(2):
            sums, mixed = at(r, i)
            value = val[r, i]
            for k in range(4):
                value = value + dif[k, r, i] * sums[k]
            for k in range(6):
                value = value + crs[k, r, i] * mixed[k]
            total[r, i] = value
            adj[r, i] = adj_in[r, i] + column(r, i)


def kernel_b(pay, flg, dif, crs, inv, total, adj_in, ra, rb, ca, cb, msg_a, msg_b, n1, n2, u1, w1, adj1, adj0, *scratch):
    beyond = outer(ra, rb, ca, cb)
    column = corner_overhang(ca, cb)

    def weight(r, i):
        x, mixed = beyond(r, i)
        value = total[r, i] + dif[0, r, i] * x
        for k in range(3):
            value = value + crs[k, r, i] * mixed[k]
        exercised = flg[r, i] == 1
        recip = inv[r, i]
        u1[r, i] = jnp.where(exercised, pay[r, i], value * recip)
        adjoint_value = adj_in[r, i] + from_wide(ra, rb, 1, r, i) + column(r, i)
        adj1[r, i] = adjoint_value
        w = jnp.where(exercised, 0.0, adjoint_value * recip)
        w1[r, i] = w
        return w

    def keep(r, i, value):
        adj0[r, i] = value

    adjoint(weight, lambda r, i: u1[r, i], dif, crs, scratch, msg_a, msg_b, n1, n2, keep)


def kernel_m(
    val, u1, flg, dif, crs, inv, total, w1, w2, cot, adj1, adj0, ra, rb, r1, r2, ca, cb, s1, s2,
    gpay, gc, part, pd, pc, out_pay, out_gc, sems, *scratch,
):
    first = inner(val, r1, r2, scratch[:4])
    beyond = outer(ra, rb, ca, cb)
    second = inner(u1, s1, s2, scratch[4:])
    column = narrow_overhang(s1, s2)
    for i in range(16):
        for r in range(2):
            sums, mixed = first(r, i)
            x, more = beyond(r, i)
            sums = (sums[0] + x, *sums[1:])
            value = total[r, i] + dif[0, r, i] * x
            for k in range(3):
                value = value + crs[k, r, i] * more[k]
            mixed = (*(mixed[k] + more[k] for k in range(3)), *mixed[3:])
            sums_2, mixed_2 = second(r, i)
            value_2 = val[r, i]
            for k in range(4):
                value_2 = value_2 + dif[k, r, i] * sums_2[k]
            for k in range(6):
                value_2 = value_2 + crs[k, r, i] * mixed_2[k]
            recip = 2.0 * inv[r, i]
            twice, twice_2 = value * recip, value_2 * recip
            w, v = w1[r, i], w2[r, i]
            for k in range(4):
                pd[k, r, i] = w * (sums[k] - twice) + v * (sums_2[k] - twice_2)
            for k in range(3):
                pc[k, r, i] = w * mixed[k] + v * mixed_2[k]
            for k in range(3, 6):
                out_gc[k - 3, r, i] = w * mixed[k] + v * mixed_2[k]
            out_pay[r, i] = jnp.where(flg[r, i] == 1, cot[r, i] + adj1[r, i], 0.0)
            part[r, i] = adj0[r, i] + w + v + column(r, i)
    copies = [pltpu.make_async_copy(out_pay, gpay, sems.at[0]), pltpu.make_async_copy(out_gc, gc.at[pl.ds(3, 3)], sems.at[1])]
    for copy in copies:
        copy.start()
    for copy in copies:
        copy.wait()


def kernel_c(side, dif, crs, inv, w2, part, pd, pc, msg, cor, *rest):
    gval, gd, gc, out_val, out_d, out_c, sems = rest[-7:]
    row, lane = rows(), lanes()
    odd = wide_odd()
    r = 1 - odd if side == 0 else odd
    high = r == 1
    sign = 0.25 * (2 * r - 1).astype(F32)
    packs = narrow_sides(cor[0], cor[1])
    right, left = (jnp.where(high, pack, lane_roll(pack, -16)) for pack in packs)
    column = columns(*(jnp.where(high, lane_roll(pack, -32), lane_roll(pack, -80)) for pack in packs))
    copies = []
    for i in range(16):
        x = msg[0, i]
        d1 = both(msg, 0, i)[1]
        d2 = up2(x, row) - down2(x, row)
        plus = jnp.where(lane == 127, lane_roll(right, 127 - i), lane_roll(x, 127))
        minus = jnp.where(lane == 0, lane_roll(left, -i), lane_roll(x, 1))
        more = (sign * d1, sign * d2, sign * (plus - minus))
        value = dif[0, r, i] * x
        for k in range(3):
            value = value + crs[k, r, i] * more[k]
        v = w2[r, i]
        change = (2.0 * inv[r, i]) * v * value
        out_d[0, i] = pd[0, r, i] + (v * x - change)
        for k in range(1, 4):
            out_d[k, i] = pd[k, r, i] - change
        for k in range(3):
            out_c[k, i] = pc[k, r, i] + v * more[k]
        out_val[i] = part[r, i] + msg[1, i] + column(0, i)
        if i % OUT_CHUNK == OUT_CHUNK - 1:
            c = i // OUT_CHUNK
            span = pl.ds(c * OUT_CHUNK, OUT_CHUNK)
            group = [
                pltpu.make_async_copy(out_d.at[:, span], gd.at[:, r, span], sems.at[c, 0]),
                pltpu.make_async_copy(out_c.at[:, span], gc.at[pl.ds(0, 3), r, span], sems.at[c, 1]),
                pltpu.make_async_copy(out_val.at[span], gval.at[r, span], sems.at[c, 2]),
            ]
            for copy in group:
                copy.start()
            copies += group
    for copy in copies:
        copy.wait()


V = pltpu.VMEM
H = pltpu.HBM


def call(kernel, outs, scratch, flops, args, spaces=None, aliases=None, limit=160):
    return pl.pallas_call(
        kernel,
        out_shape=[jax.ShapeDtypeStruct(out[0], out[2] if len(out) > 2 else F32) for out in outs],
        in_specs=[pl.BlockSpec(memory_space=space) for space in (spaces or [V] * len(args))],
        out_specs=[pl.BlockSpec(memory_space=out[1]) for out in outs],
        scratch_shapes=scratch,
        input_output_aliases=aliases or {},
        cost_estimate=pl.CostEstimate(flops=flops, bytes_accessed=4 << 20, transcendentals=0),
        compiler_params=pltpu.CompilerParams(vmem_limit_bytes=limit << 18),
    )(*args)


def swap(x, axis, odd):
    pairs = []
    for i in range(odd, lax.axis_size(axis) - 1, 2):
        pairs += [(i, i + 1), (i + 1, i)]
    return lax.ppermute(x, axis, pairs)


def exchange(msg_a, msg_b, n1, n2):
    r2 = swap(n2, "narrow", 1)
    rb = swap(msg_b, "wide", 1)
    r1 = swap(n1, "narrow", 0)
    ra = swap(msg_a, "wide", 0)
    corners = jnp.stack([r1, r2])
    cb = swap(corners, "wide", 1)
    ca = swap(corners, "wide", 0)
    return ra, rb, r1, r2, ca, cb


def body(value_in, payoff, diffusion, cross_terms, flags, cotangent):
    four, six = (4, *BLOCK), (6, *BLOCK)
    message = (2, 16, *TILE)
    sends = [(message, V), (message, V), (TILE, V), (TILE, V)]
    block = (BLOCK, V)
    msg_a, msg_b, n1, n2, inv, w2, adj, cot, flg, val = call(
        kernel_a,
        [*sends, block, block, block, block, (BLOCK, V, jnp.int32), block],
        [pltpu.VMEM(four, F32), pltpu.VMEM(six, F32), pltpu.SemaphoreType.DMA((16 // IN_CHUNK, 5)), *ADJOINT_SCRATCH],
        40 << 16,
        (cotangent, flags[0], diffusion, cross_terms, value_in),
        [H] * 5,
        limit=207,
    )
    ra, rb, r1, r2, ca, cb = exchange(msg_a, msg_b, n1, n2)
    total, adj = call(kernel_p, [block, block], INNER_SCRATCH, 40 << 16, (val, diffusion, cross_terms, adj, r1, r2))
    msg_a, msg_b, n1, n2, u1, w1, adj1, adj0 = call(
        kernel_b,
        [*sends, block, block, block, block],
        ADJOINT_SCRATCH,
        60 << 16,
        (payoff, flg, diffusion, cross_terms, inv, total, adj, ra, rb, ca, cb),
    )
    sa, sb, s1, s2, da, db = exchange(msg_a, msg_b, n1, n2)
    gpay, gc, part, pd, pc = call(
        kernel_m,
        [(BLOCK, H), (six, H), block, (four, V), ((3, *BLOCK), V)],
        [pltpu.VMEM(BLOCK, F32), pltpu.VMEM((3, *BLOCK), F32), pltpu.SemaphoreType.DMA((2,)), *INNER_SCRATCH, *INNER_SCRATCH],
        120 << 16,
        (val, u1, flg, diffusion, cross_terms, inv, total, w1, w2, cot, adj1, adj0, ra, rb, r1, r2, ca, cb, s1, s2),
    )
    half = (16, *TILE)
    scratch = [pltpu.VMEM(half, F32), pltpu.VMEM((4, *half), F32), pltpu.VMEM((3, *half), F32), pltpu.SemaphoreType.DMA((16 // OUT_CHUNK, 3))]
    outs = [(BLOCK, H), (four, H), (six, H)]
    given = (diffusion, cross_terms, inv, w2, part, pd, pc)
    gval, gd, gc = call(functools.partial(kernel_c, 0), outs, scratch, 20 << 16, (*given, sa, da, gc), [V] * 9 + [H], {9: 2})
    gval, gd, gc = call(
        functools.partial(kernel_c, 1), outs, scratch, 20 << 16, (*given, sb, db, gval, gd, gc), [V] * 9 + [H] * 3, {9: 0, 10: 1, 11: 2}
    )
    return gval, gpay, gd, gc


def solution(mesh):
    field = P("wide", None, None, "narrow")
    stack = P(None, "wide", None, None, "narrow")
    return jax.shard_map(
        body, mesh=mesh, in_specs=(field, field, stack, stack, stack, field), out_specs=(field, field, stack, stack), check_vma=False
    )
```

```python
import functools

import jax
import jax.numpy as jnp
from jax import lax
from jax.experimental import pallas as pl
from jax.experimental.pallas import tpu as pltpu
from jax.sharding import PartitionSpec as P

F32 = jnp.float32
TILE = (16, 128)
BLOCK = (2, 16, 16, 128)
OUT_CHUNK = 8
IN_CHUNK = 8


def lanes():
    return lax.broadcasted_iota(jnp.int32, TILE, 1)


def rows():
    return lax.broadcasted_iota(jnp.int32, TILE, 0)


def lane_roll(x, shift):
    shift = shift % 128
    return x if shift == 0 else pltpu.roll(x, shift, 1)


def up2(x, row):
    return jnp.where(row == 15, 0.0, pltpu.roll(x, 15, 0))


def down2(x, row):
    return jnp.where(row == 0, 0.0, pltpu.roll(x, 1, 0))


def both(ref, r, i):
    if i == 0:
        return ref[r, 1], ref[r, 1]
    if i == 15:
        return ref[r, 14], -ref[r, 14]
    return ref[r, i + 1] + ref[r, i - 1], ref[r, i + 1] - ref[r, i - 1]


def wide_odd():
    return lax.rem(lax.axis_index("wide"), 2)


def narrow_odd():
    return lax.rem(lax.axis_index("narrow"), 2)


def narrow_sides(first, second):
    even = narrow_odd() == 0
    return jnp.where(even, first, second), jnp.where(even, second, first)


def corner_sides(cor_a, cor_b):
    even = wide_odd() == 0
    a_right, a_left = narrow_sides(cor_a[0], cor_a[1])
    b_right, b_left = narrow_sides(cor_b[0], cor_b[1])
    low = jnp.where(even, b_right, a_right), jnp.where(even, b_left, a_left)
    high = jnp.where(even, a_right, b_right), jnp.where(even, a_left, b_left)
    return low, high


def from_wide(ra, rb, part, r, i):
    even = wide_odd() == 0
    low, high = (rb, ra) if r == 0 else (ra, rb)
    return jnp.where(even, low[part, i], high[part, i])


def adjoint(w_of, u_of, dif, crs, parts, scratch, msg_a, msg_b, n1, n2):
    q0s, q1s, p01s, p12s, x2s, y2s, x3s, y3s = parts
    p13s, p02s, p03s = scratch
    row, lane = rows(), lanes()
    for i in range(16):
        w = [w_of(r, i) for r in range(2)]
        h = [0.25 * w[r] for r in range(2)]
        p02 = [crs[1, r, i] * h[r] for r in range(2)]
        p03 = [crs[2, r, i] * h[r] for r in range(2)]
        for r in range(2):
            q0s[r, i] = dif[0, r, i] * w[r]
            q1s[r, i] = dif[1, r, i] * w[r]
            p01s[r, i] = crs[0, r, i] * h[r]
            p12s[r, i] = crs[3, r, i] * h[r]
            p13s[r, i] = crs[4, r, i] * h[r]
            p02s[r, i] = p02[r]
            p03s[r, i] = p03[r]
            q2 = dif[2, r, i] * w[r]
            e02 = p02[1] if r == 0 else -p02[0]
            x2s[r, i] = q2 + e02
            y2s[r, i] = q2 - e02
            q3 = dif[3, r, i] * w[r]
            p23 = crs[5, r, i] * h[r]
            e3 = (p03[1] if r == 0 else -p03[0]) + (up2(p23, row) - down2(p23, row))
            x3s[r, i] = q3 + e3
            y3s[r, i] = q3 - e3
    odd = wide_odd()
    row_a = 1 - odd
    row_b = odd
    sign_a = (2 * odd - 1).astype(F32)
    left = jnp.zeros(TILE, F32)
    right = jnp.zeros(TILE, F32)

    def put(packed, value, source, column):
        return jnp.where(lane == column, lane_roll(value, column - source), packed)

    for i in range(16):
        for r in range(2):
            u = u_of(r, i)
            left = put(left, u, 0, r * 16 + i)
            right = put(right, u, 127, r * 16 + i)
            f13 = both(p13s, r, i)[1]
            x3 = x3s[r, i] + f13
            y3 = y3s[r, i] - f13
            x3s[r, i] = x3
            y3s[r, i] = y3
            left = put(left, x3, 0, 48 + r * 16 + i)
            right = put(right, y3, 127, 48 + r * 16 + i)
        p0, p1 = p03s[0, i], p03s[1, i]
        left = put(left, p0, 0, 32 + i)
        right = put(right, -p0, 127, 32 + i)
        left = put(left, -p1, 0, 80 + i)
        right = put(right, p1, 127, 80 + i)
        for msg, at, sign in ((msg_a, row_a, sign_a), (msg_b, row_b, -sign_a)):
            p02, p03 = p02s[at, i], p03s[at, i]
            d = both(p01s, at, i)[1]
            d = d + up2(p02, row) - down2(p02, row)
            d = d + jnp.where(lane == 127, 0.0, lane_roll(p03, 127)) - jnp.where(lane == 0, 0.0, lane_roll(p03, 1))
            msg[1, i] = q0s[at, i] + sign * d
            msg[0, i] = u_of(at, i)
    even = narrow_odd() == 0
    n1[...] = jnp.where(even, right, left)
    n2[...] = jnp.where(even, left, right)


def own_adjoint(parts):
    q0s, q1s, p01s, p12s, x2s, y2s, x3s, y3s = parts
    row, lane = rows(), lanes()

    def at(r, i):
        f12 = both(p12s, r, i)[1]
        x3, y3 = x3s[r, i], y3s[r, i]
        x2 = x2s[r, i] + f12
        y2 = y2s[r, i] - f12
        e01 = both(p01s, 1 - r, i)[1]
        total = q0s[1 - r, i] + both(q1s, r, i)[0]
        total = total + e01 if r == 0 else total - e01
        total = total + up2(x2, row) + down2(y2, row)
        return total + jnp.where(lane == 127, 0.0, lane_roll(x3, 127)) + jnp.where(lane == 0, 0.0, lane_roll(y3, 1))

    return at


def inner(us, r1, r2, scratch):
    d2s, d3s, n2s, n3s = scratch
    row, lane = rows(), lanes()
    from_right, from_left = narrow_sides(r1[...], r2[...])
    for i in range(16):
        for r in range(2):
            x = us[r, i]
            at = r * 16 + i
            plus = jnp.where(lane == 127, lane_roll(from_right, 127 - at), lane_roll(x, 127))
            minus = jnp.where(lane == 0, lane_roll(from_left, -at), lane_roll(x, 1))
            above, below = up2(x, row), down2(x, row)
            d3s[r, i] = plus - minus
            d2s[r, i] = above - below
            n3s[r, i] = plus + minus
            n2s[r, i] = above + below

    def at(r, i):
        d3 = d3s[r, i]
        sign = 0.25 if r == 0 else -0.25
        sums = (us[1 - r, i], both(us, r, i)[0], n2s[r, i], n3s[r, i])
        mixed = (
            sign * both(us, 1 - r, i)[1],
            sign * d2s[1 - r, i],
            sign * d3s[1 - r, i],
            0.25 * both(d2s, r, i)[1],
            0.25 * both(d3s, r, i)[1],
            0.25 * (up2(d3, row) - down2(d3, row)),
        )
        return sums, mixed

    return at


def outer(ra, rb, ca, cb):
    row, lane = rows(), lanes()
    low, high = corner_sides(ca, cb)

    def at(r, i):
        x = from_wide(ra, rb, 0, r, i)
        (pack_right, pack_left), base = (low, 16) if r == 0 else (high, 0)
        sign = -0.25 if r == 0 else 0.25
        if i == 0:
            d1 = from_wide(ra, rb, 0, r, 1)
        elif i == 15:
            d1 = -from_wide(ra, rb, 0, r, 14)
        else:
            d1 = from_wide(ra, rb, 0, r, i + 1) - from_wide(ra, rb, 0, r, i - 1)
        d2 = up2(x, row) - down2(x, row)
        plus = jnp.where(lane == 127, lane_roll(pack_right, 127 - base - i), lane_roll(x, 127))
        minus = jnp.where(lane == 0, lane_roll(pack_left, -base - i), lane_roll(x, 1))
        return x, (sign * d1, sign * d2, sign * (plus - minus))

    return at


def columns(right, left):
    lane = lanes()

    def at(r, i):
        k = r * 16 + i
        return jnp.where(lane == 127, lane_roll(right, 127 - k), jnp.where(lane == 0, lane_roll(left, -k), 0.0))

    return at


def narrow_overhang(r1, r2):
    right, left = narrow_sides(r1[...], r2[...])
    return columns(lane_roll(right, -48), lane_roll(left, -48))


def corner_overhang(ca, cb):
    lane = lanes()
    low, high = corner_sides(ca, cb)
    merged = [jnp.where(lane < 16, lane_roll(low[k], -80), lane_roll(high[k], -16)) for k in range(2)]
    return columns(*merged)


ADJOINT_SCRATCH = [pltpu.VMEM(BLOCK, F32)] * 3
PARTS = 8
INNER_SCRATCH = [pltpu.VMEM(BLOCK, F32)] * 4


def kernel_a(cot_h, flg_h, dif_h, crs_h, val_h, msg_a, msg_b, n1, n2, inv, w2, cot, flg, val, *rest):
    parts, (dif, crs, sems, *scratch) = rest[:PARTS], rest[PARTS:]
    copies = []
    for c in range(16 // IN_CHUNK):
        span = pl.ds(c * IN_CHUNK, IN_CHUNK)
        group = []
        for k, (src, dst) in enumerate(((cot_h, cot), (flg_h, flg), (val_h, val))):
            group.append(pltpu.make_async_copy(src.at[:, span], dst.at[:, span], sems.at[c, k]))
        for k, (src, dst) in enumerate(((dif_h, dif), (crs_h, crs))):
            group.append(pltpu.make_async_copy(src.at[:, :, span], dst.at[:, :, span], sems.at[c, 3 + k]))
        for copy in group:
            copy.start()
        copies.append(group)

    def weight(r, i):
        if r == 0 and i % IN_CHUNK == 0:
            for copy in copies[i // IN_CHUNK]:
                copy.wait()
        recip = 1.0 / (1.0 + 2.0 * (dif[0, r, i] + dif[1, r, i] + dif[2, r, i] + dif[3, r, i]))
        inv[r, i] = recip
        w = jnp.where(flg[r, i] == 1, 0.0, cot[r, i] * recip)
        w2[r, i] = w
        return w

    adjoint(weight, lambda r, i: val[r, i], dif, crs, parts, scratch, msg_a, msg_b, n1, n2)


def kernel_p(val, dif, crs, r1, r2, *rest):
    own, (total, adj, *scratch) = own_adjoint(rest[:PARTS]), rest[PARTS:]
    at = inner(val, r1, r2, scratch)
    column = narrow_overhang(r1, r2)
    for i in range(16):
        for r in range(2):
            sums, mixed = at(r, i)
            value = val[r, i]
            for k in range(4):
                value = value + dif[k, r, i] * sums[k]
            for k in range(6):
                value = value + crs[k, r, i] * mixed[k]
            total[r, i] = value
            adj[r, i] = own(r, i) + column(r, i)


def kernel_b(pay, flg, dif, crs, inv, total, adj_in, ra, rb, ca, cb, msg_a, msg_b, n1, n2, u1, w1, adj1, *rest):
    beyond = outer(ra, rb, ca, cb)
    column = corner_overhang(ca, cb)

    def weight(r, i):
        x, mixed = beyond(r, i)
        value = total[r, i] + dif[0, r, i] * x
        for k in range(3):
            value = value + crs[k, r, i] * mixed[k]
        exercised = flg[r, i] == 1
        recip = inv[r, i]
        u1[r, i] = jnp.where(exercised, pay[r, i], value * recip)
        adjoint_value = adj_in[r, i] + from_wide(ra, rb, 1, r, i) + column(r, i)
        adj1[r, i] = adjoint_value
        w = jnp.where(exercised, 0.0, adjoint_value * recip)
        w1[r, i] = w
        return w

    adjoint(weight, lambda r, i: u1[r, i], dif, crs, rest[:PARTS], rest[PARTS:], msg_a, msg_b, n1, n2)


def kernel_m(
    val, u1, flg, dif, crs, inv, total, w1, w2, cot, adj1, ra, rb, r1, r2, ca, cb, s1, s2, *rest
):
    own, (gpay, gc, part, pd, pc, out_pay, out_gc, sems, *scratch) = own_adjoint(rest[:PARTS]), rest[PARTS:]
    first = inner(val, r1, r2, scratch[:4])
    beyond = outer(ra, rb, ca, cb)
    second = inner(u1, s1, s2, scratch[4:])
    column = narrow_overhang(s1, s2)
    for i in range(16):
        for r in range(2):
            sums, mixed = first(r, i)
            x, more = beyond(r, i)
            sums = (sums[0] + x, *sums[1:])
            value = total[r, i] + dif[0, r, i] * x
            for k in range(3):
                value = value + crs[k, r, i] * more[k]
            mixed = (*(mixed[k] + more[k] for k in range(3)), *mixed[3:])
            sums_2, mixed_2 = second(r, i)
            value_2 = val[r, i]
            for k in range(4):
                value_2 = value_2 + dif[k, r, i] * sums_2[k]
            for k in range(6):
                value_2 = value_2 + crs[k, r, i] * mixed_2[k]
            recip = 2.0 * inv[r, i]
            twice, twice_2 = value * recip, value_2 * recip
            w, v = w1[r, i], w2[r, i]
            for k in range(4):
                pd[k, r, i] = w * (sums[k] - twice) + v * (sums_2[k] - twice_2)
            for k in range(3):
                pc[k, r, i] = w * mixed[k] + v * mixed_2[k]
            for k in range(3, 6):
                out_gc[k - 3, r, i] = w * mixed[k] + v * mixed_2[k]
            out_pay[r, i] = jnp.where(flg[r, i] == 1, cot[r, i] + adj1[r, i], 0.0)
            part[r, i] = own(r, i) + w + v + column(r, i)
    copies = [pltpu.make_async_copy(out_pay, gpay, sems.at[0]), pltpu.make_async_copy(out_gc, gc.at[pl.ds(3, 3)], sems.at[1])]
    for copy in copies:
        copy.start()
    for copy in copies:
        copy.wait()


def kernel_c(side, dif, crs, inv, w2, part, pd, pc, msg, cor, *rest):
    gval, gd, gc, out_val, out_d, out_c, sems = rest[-7:]
    row, lane = rows(), lanes()
    odd = wide_odd()
    r = 1 - odd if side == 0 else odd
    high = r == 1
    sign = 0.25 * (2 * r - 1).astype(F32)
    packs = narrow_sides(cor[0], cor[1])
    right, left = (jnp.where(high, pack, lane_roll(pack, -16)) for pack in packs)
    column = columns(*(jnp.where(high, lane_roll(pack, -32), lane_roll(pack, -80)) for pack in packs))
    copies = []
    for i in range(16):
        x = msg[0, i]
        d1 = both(msg, 0, i)[1]
        d2 = up2(x, row) - down2(x, row)
        plus = jnp.where(lane == 127, lane_roll(right, 127 - i), lane_roll(x, 127))
        minus = jnp.where(lane == 0, lane_roll(left, -i), lane_roll(x, 1))
        more = (sign * d1, sign * d2, sign * (plus - minus))
        value = dif[0, r, i] * x
        for k in range(3):
            value = value + crs[k, r, i] * more[k]
        v = w2[r, i]
        change = (2.0 * inv[r, i]) * v * value
        out_d[0, i] = pd[0, r, i] + (v * x - change)
        for k in range(1, 4):
            out_d[k, i] = pd[k, r, i] - change
        for k in range(3):
            out_c[k, i] = pc[k, r, i] + v * more[k]
        out_val[i] = part[r, i] + msg[1, i] + column(0, i)
        if i % OUT_CHUNK == OUT_CHUNK - 1:
            c = i // OUT_CHUNK
            span = pl.ds(c * OUT_CHUNK, OUT_CHUNK)
            group = [
                pltpu.make_async_copy(out_d.at[:, span], gd.at[:, r, span], sems.at[c, 0]),
                pltpu.make_async_copy(out_c.at[:, span], gc.at[pl.ds(0, 3), r, span], sems.at[c, 1]),
                pltpu.make_async_copy(out_val.at[span], gval.at[r, span], sems.at[c, 2]),
            ]
            for copy in group:
                copy.start()
            copies += group
    for copy in copies:
        copy.wait()


V = pltpu.VMEM
H = pltpu.HBM


def call(kernel, outs, scratch, flops, args, spaces=None, aliases=None, limit=160):
    return pl.pallas_call(
        kernel,
        out_shape=[jax.ShapeDtypeStruct(out[0], out[2] if len(out) > 2 else F32) for out in outs],
        in_specs=[pl.BlockSpec(memory_space=space) for space in (spaces or [V] * len(args))],
        out_specs=[pl.BlockSpec(memory_space=out[1]) for out in outs],
        scratch_shapes=scratch,
        input_output_aliases=aliases or {},
        cost_estimate=pl.CostEstimate(flops=flops, bytes_accessed=4 << 20, transcendentals=0),
        compiler_params=pltpu.CompilerParams(vmem_limit_bytes=limit << 18),
    )(*args)


def swap(x, axis, odd):
    pairs = []
    for i in range(odd, lax.axis_size(axis) - 1, 2):
        pairs += [(i, i + 1), (i + 1, i)]
    return lax.ppermute(x, axis, pairs)


def exchange(msg_a, msg_b, n1, n2):
    r2 = swap(n2, "narrow", 1)
    rb = swap(msg_b, "wide", 1)
    r1 = swap(n1, "narrow", 0)
    ra = swap(msg_a, "wide", 0)
    corners = jnp.stack([r1, r2])
    cb = swap(corners, "wide", 1)
    ca = swap(corners, "wide", 0)
    return ra, rb, r1, r2, ca, cb


def body(value_in, payoff, diffusion, cross_terms, flags, cotangent):
    four, six = (4, *BLOCK), (6, *BLOCK)
    message = (2, 16, *TILE)
    sends = [(message, V), (message, V), (TILE, V), (TILE, V)]
    block = (BLOCK, V)
    msg_a, msg_b, n1, n2, inv, w2, cot, flg, val, *parts = call(
        kernel_a,
        [*sends, block, block, block, (BLOCK, V, jnp.int32), block, *[block] * PARTS],
        [pltpu.VMEM(four, F32), pltpu.VMEM(six, F32), pltpu.SemaphoreType.DMA((16 // IN_CHUNK, 5)), *ADJOINT_SCRATCH],
        40 << 16,
        (cotangent, flags[0], diffusion, cross_terms, value_in),
        [H] * 5,
        limit=200,
    )
    ra, rb, r1, r2, ca, cb = exchange(msg_a, msg_b, n1, n2)
    total, adj = call(kernel_p, [block, block], INNER_SCRATCH, 40 << 16, (val, diffusion, cross_terms, r1, r2, *parts))
    msg_a, msg_b, n1, n2, u1, w1, adj1, *parts = call(
        kernel_b,
        [*sends, block, block, block, *[block] * PARTS],
        ADJOINT_SCRATCH,
        60 << 16,
        (payoff, flg, diffusion, cross_terms, inv, total, adj, ra, rb, ca, cb),
    )
    sa, sb, s1, s2, da, db = exchange(msg_a, msg_b, n1, n2)
    gpay, gc, part, pd, pc = call(
        kernel_m,
        [(BLOCK, H), (six, H), block, (four, V), ((3, *BLOCK), V)],
        [pltpu.VMEM(BLOCK, F32), pltpu.VMEM((3, *BLOCK), F32), pltpu.SemaphoreType.DMA((2,)), *INNER_SCRATCH, *INNER_SCRATCH],
        120 << 16,
        (val, u1, flg, diffusion, cross_terms, inv, total, w1, w2, cot, adj1, ra, rb, r1, r2, ca, cb, s1, s2, *parts),
    )
    half = (16, *TILE)
    scratch = [pltpu.VMEM(half, F32), pltpu.VMEM((4, *half), F32), pltpu.VMEM((3, *half), F32), pltpu.SemaphoreType.DMA((16 // OUT_CHUNK, 3))]
    outs = [(BLOCK, H), (four, H), (six, H)]
    given = (diffusion, cross_terms, inv, w2, part, pd, pc)
    gval, gd, gc = call(functools.partial(kernel_c, 0), outs, scratch, 20 << 16, (*given, sa, da, gc), [V] * 9 + [H], {9: 2})
    gval, gd, gc = call(
        functools.partial(kernel_c, 1), outs, scratch, 20 << 16, (*given, sb, db, gval, gd, gc), [V] * 9 + [H] * 3, {9: 0, 10: 1, 11: 2}
    )
    return gval, gpay, gd, gc


def solution(mesh):
    field = P("wide", None, None, "narrow")
    stack = P(None, "wide", None, None, "narrow")
    return jax.shard_map(
        body, mesh=mesh, in_specs=(field, field, stack, stack, stack, field), out_specs=(field, field, stack, stack), check_vma=False
    )
```
